64 devices in a mesh: rep: 4 (over x, y), dp: 16 (over z, core).
Axes of the slice: x: 2, y: 2, z: 8, core: 2. Of those that a mesh axis runs over, the one named last changes fastest.
The devices are a block of a 4x4x8 slice.
Arguments:
- a: bfloat16 [64, 4, 2048, 896], P(('rep', 'dp')), parts along dimension 0
- g: bfloat16 [64, 4, 2048, 4736], P(('rep', 'dp')), parts along dimension 0
Outputs:
- output: bfloat16 [16, 896, 4736], P('rep'), parts along dimension 0
There are 4 independent parts. The reference program is written for one: setup_inputs(seed, part) draws one part's arguments, and reference() takes and returns one part's arrays. A program takes and returns all parts, laid end to end along the dimension named above; each array names one.
All inputs are finite; a program needn't handle non-finite values.
Results may differ from the reference program's by a relative error of at most 0.012.
Values are sent between devices in bfloat16 or wider.
A program may use at most 768 MiB of HBM per device.

```python
import jax
import jax.numpy as jnp
from jax import lax

DEVICES = 16
MATRICES = 4
TOKENS = 2048
D = 896
FF = 4736


def setup_inputs(seed: int = 0, part: int = 0) -> dict:
    ka, kg, ks = (jax.random.fold_in(k, part) for k in jax.random.split(jax.random.key(seed), 3))
    size = 2.0 ** jax.random.uniform(ks, (DEVICES, MATRICES, 1, 1), jnp.float32, -1.0, 1.0)
    a = jax.random.normal(ka, (DEVICES, MATRICES, TOKENS, D), jnp.float32)
    g = size * jax.random.normal(kg, (DEVICES, MATRICES, TOKENS, FF), jnp.float32) * (DEVICES * TOKENS) ** -0.5
    return {"a": a.astype(jnp.bfloat16), "g": g.astype(jnp.bfloat16)}


def reference(a, g):
    def take(so_far, one):
        return so_far + jnp.einsum("ntd,ntf->ndf", *one, preferred_element_type=jnp.float32), None

    return lax.scan(take, jnp.zeros((MATRICES, D, FF), jnp.float32), (a, g))[0].astype(jnp.bfloat16)
```

```python
import functools

import jax
import jax.numpy as jnp
from jax import lax
from jax.experimental import pallas as pl
from jax.experimental.pallas import tpu as pltpu
from jax.sharding import PartitionSpec as P

MESH = pl.DeviceIdType.MESH
CORES = 2
TILE = 512
KBLOCK = 256
STAGES = 4
WRITES = 16


def kernel(chips, a_ref, g_ref, x_ref, stage, at, gp, go, acc, pbuf, pin,
           stage_sem, gp_sem, go_sem, psend, precv, osend, rrecv, gsend, dsend, grecv, drecv, clear):
    _, mats, tokens, depth = a_ref.shape
    width = g_ref.shape[3]
    rows = at.shape[1]
    per_mat = depth // rows
    full = width // TILE
    widths = [TILE] * full + ([width - full * TILE] if width % TILE else [])
    tiles = len(widths)
    total = chips * tiles

    dp = lax.axis_index("dp")
    z, c = dp // CORES, dp % CORES
    d = 1 - 2 * c
    nxt = lax.rem(z + d + chips, chips) * CORES + c
    prv = lax.rem(z - d + chips, chips) * CORES + c
    par = z * CORES + 1 - c

    def mine(s):
        return lax.rem(z - d * (s + 1) + 2 * chips, chips)

    def theirs(s):
        return lax.rem(z + d * (s + 1) + 2 * chips, chips)

    def columns(j, w):
        return pl.ds(j * TILE if isinstance(j, int) else pl.multiple_of(j * TILE, TILE), w)

    def g_copy(buf, sem, mat, j, w, slot):
        return pltpu.make_async_copy(g_ref.at[0, mat, :, columns(j, w)], buf.at[slot, :, pl.ds(0, w)], sem.at[slot])

    def g_start(buf, sem, chunk, t):
        s, j = t // tiles, t % tiles
        mat = chunk(s) * CORES // per_mat

        @pl.when((t < total) & (j < full))
        def _():
            g_copy(buf, sem, mat, j, TILE, t % 2).start()

        if tiles > full:
            @pl.when((t < total) & (j == full))
            def _():
                g_copy(buf, sem, mat, full, widths[full], t % 2).start()

    some = tokens // STAGES

    def a_copy(mat, k):
        return pltpu.make_async_copy(
            a_ref.at[0, mat, pl.ds(pl.multiple_of(k * some, some), some)], stage.at[k], stage_sem.at[k])

    def transpose(i):
        @pl.loop(0, STAGES)
        def _(k):
            a_copy(order[i], k).wait()
            for b in range(some // KBLOCK):
                span = pl.ds(pl.multiple_of(k * some + b * KBLOCK, KBLOCK), KBLOCK)
                block = stage[k, b * KBLOCK:(b + 1) * KBLOCK, :].T
                for r in range(per_mat):
                    at[order[i] * per_mat + r, :, span] = block[r * rows:(r + 1) * rows]
            if i + 1 < mats:
                a_copy(order[i + 1], k).start()

    def to_partner(t, j, w):
        return pltpu.make_async_remote_copy(
            pbuf.at[j, :, pl.ds(0, w)], pin.at[t % 4, :, pl.ds(0, w)], psend.at[j], precv.at[t % 4],
            device_id={"dp": par}, device_id_type=MESH)

    def place(chunk, core, j, w):
        return x_ref.at[pl.ds(pl.multiple_of((chunk * CORES + core) * rows, rows), rows), columns(j, w)]

    def to_next(s, j, w):
        here = place(mine(s), c, j, w)
        return pltpu.make_async_remote_copy(
            here, here, osend.at[j], rrecv.at[s, j], device_id={"dp": nxt}, device_id_type=MESH)

    def gather(s, j, w):
        here = place(lax.rem(z - d * s + 2 * chips, chips), c, j, w)
        return pltpu.make_async_remote_copy(
            here, here, gsend, grecv.at[s, j], device_id={"dp": nxt}, device_id_type=MESH)

    def share(s, j, w):
        here = place(lax.rem(z - d * s + 2 * chips, chips), c, j, w)
        return pltpu.make_async_remote_copy(
            here, here, dsend, drecv.at[s, j], device_id={"dp": par}, device_id_type=MESH)

    def partner_term(s, j, w):
        t = s * tiles + j
        slot = t % 2
        chunk = theirs(s)
        g_copy(gp, gp_sem, chunk * CORES // per_mat, j, w, slot).wait()

        @pl.when(s > 0)
        def _():
            to_partner(t, j, w).wait_send()

        pbuf[j, :, :w] = jnp.dot(
            at[chunk * CORES + 1 - c], gp[slot, :, :w], preferred_element_type=jnp.float32).astype(jnp.bfloat16)
        to_partner(t, j, w).start()

    def own_term(s, j, w):
        t = s * tiles + j
        slot = t % 2
        chunk = mine(s)
        g_copy(go, go_sem, chunk * CORES // per_mat, j, w, slot).wait()
        acc[:, :w] = jnp.dot(at[chunk * CORES + c], go[slot, :, :w], preferred_element_type=jnp.float32)
        to_partner(t, j, w).wait_recv()

        here = place(chunk, c, j, w)

        @pl.when(s == 0)
        def _():
            here[...] = (acc[:, :w] + pin[t % 4, :, :w].astype(jnp.float32)).astype(jnp.bfloat16)

        @pl.when(s > 0)
        def _():
            to_next(s - 1, j, w).wait()
            here[...] = (
                acc[:, :w] + pin[t % 4, :, :w].astype(jnp.float32) + here[...].astype(jnp.float32)
            ).astype(jnp.bfloat16)

        @pl.when(s < chips - 1)
        def _():
            to_next(s, j, w).start()

        @pl.when(s == chips - 1)
        def _():
            gather(0, j, w).start()
            share(0, j, w).start()

    barrier = pltpu.get_barrier_semaphore()
    for who in (nxt, prv, par):
        pl.semaphore_signal(barrier, inc=1, device_id={"dp": who}, device_id_type=MESH)

    order = [theirs(0) * CORES // per_mat, mine(0) * CORES // per_mat]
    early = lax.rem((z + chips - 1) // CORES, mats)
    order += [lax.rem(early + i, mats) for i in range(2, mats)]
    for k in range(STAGES):
        a_copy(order[0], k).start()
    g_start(gp, gp_sem, theirs, 0)
    g_start(go, go_sem, mine, 0)
    g_start(gp, gp_sem, theirs, 1)
    transpose(0)
    pl.semaphore_wait(barrier, 3)
    partner_term(0, 0, widths[0])
    transpose(1)

    def step(s, j, w, w_after):
        t = s * tiles + j
        g_start(gp, gp_sem, theirs, t + 2)
        g_start(go, go_sem, mine, t + 1)
        if w_after is None:
            @pl.when(s < chips - 1)
            def _():
                partner_term(s + 1, 0, widths[0])
        else:
            partner_term(s, j + 1, w_after)
        own_term(s, j, w)

    @pl.loop(0, chips)
    def _(s):
        @pl.loop(0, full - 1)
        def _(j):
            step(s, j, TILE, TILE)
            for i in range(2, mats):
                @pl.when((s == 0) & (j == 2 * i - 2))
                def _():
                    transpose(i)

        for j in range(full - 1, tiles):
            step(s, j, widths[j], widths[j + 1] if j + 1 < tiles else None)

    pl.semaphore_signal(clear, inc=1, device_id={"dp": prv}, device_id_type=MESH)
    for j, w in enumerate(widths):
        to_partner((chips - 1) * tiles + j, j, w).wait_send()

    @pl.loop(1, chips)
    def _(s):
        @pl.when(s == chips - 3)
        def _():
            pl.semaphore_wait(clear, 1)

        for j, w in enumerate(widths):
            gather(s - 1, j, w).wait_recv()

            @pl.when(s < chips - 1)
            def _():
                gather(s, j, w).start()

            share(s, j, w).start()

    @pl.loop(0, chips)
    def _(s):
        for j, w in enumerate(widths):
            share(s, j, w).wait_recv()

    def all_bytes(chunks, sem):
        part = x_ref.at[pl.ds(0, chunks * rows)]
        pltpu.make_async_copy(part, part, sem).wait()

    all_bytes(chips - 1, gsend)
    all_bytes(chips, dsend)


def writer(x_ref, o_ref, sem):
    part = x_ref.shape[0] // WRITES
    copies = [
        pltpu.make_async_copy(x_ref.at[pl.ds(i * part, part)], o_ref.at[pl.ds(i * part, part)], sem.at[i])
        for i in range(WRITES)
    ]
    for copy in copies:
        copy.start()
    for copy in copies:
        copy.wait()


def solution(mesh):
    members = mesh.shape["dp"]
    chips = members // CORES

    def body(a, g):
        _, mats, tokens, depth = a.shape
        width = g.shape[3]
        rows = mats * depth // members
        tiles = pl.cdiv(width, TILE)
        bf16, f32, dma = jnp.bfloat16, jnp.float32, pltpu.SemaphoreType.DMA
        sums = pl.pallas_call(
            functools.partial(kernel, chips),
            out_shape=pltpu.VMEM((mats * depth, width), bf16),
            in_specs=[pl.BlockSpec(memory_space=pl.ANY)] * 2,
            out_specs=pl.BlockSpec(memory_space=pltpu.VMEM),
            scratch_shapes=[
                pltpu.VMEM((STAGES, tokens // STAGES, depth), bf16),
                pltpu.VMEM((members, rows, tokens), bf16),
                pltpu.VMEM((2, tokens, TILE), bf16),
                pltpu.VMEM((2, tokens, TILE), bf16),
                pltpu.VMEM((rows, TILE), f32),
                pltpu.VMEM((tiles, rows, TILE), bf16),
                pltpu.VMEM((4, rows, TILE), bf16),
                dma((STAGES,)), dma((2,)), dma((2,)),
                dma((tiles,)), dma((4,)), dma((tiles,)), dma((chips - 1, tiles)),
                dma, dma,
                dma((chips - 1, tiles)), dma((chips, tiles)),
                pltpu.SemaphoreType.REGULAR,
            ],
            compiler_params=pltpu.CompilerParams(
                collective_id=0, has_side_effects=True, vmem_limit_bytes=30 * 2**20),
        )(a, g)
        out = pl.pallas_call(
            writer,
            out_shape=jax.ShapeDtypeStruct((mats * depth, width), bf16),
            in_specs=[pl.BlockSpec(memory_space=pltpu.VMEM)],
            out_specs=pl.BlockSpec(memory_space=pl.ANY),
            scratch_shapes=[dma((WRITES,))],
            compiler_params=pltpu.CompilerParams(vmem_limit_bytes=2**20),
        )(sums)
        return out.reshape(mats, depth, width)

    part = P(("rep", "dp"))
    return jax.shard_map(body, mesh=mesh, in_specs=(part, part), out_specs=P("rep"), check_vma=False)
```

```python
import functools

import jax
import jax.numpy as jnp
from jax import lax
from jax.experimental import pallas as pl
from jax.experimental.pallas import tpu as pltpu
from jax.sharding import PartitionSpec as P

MESH = pl.DeviceIdType.MESH
CORES = 2
TILE = 512
KBLOCK = 256
STAGES = 4
LANES = 128
WRITES = 16


def kernel(chips, a_ref, g_ref, x_ref, stage, at, gp, go, acc, pbuf, pin,
           stage_sem, early_sem, gp_sem, go_sem, psend, precv, osend, rrecv, gsend, dsend, grecv, drecv, clear):
    _, mats, tokens, depth = a_ref.shape
    width = g_ref.shape[3]
    rows = at.shape[1]
    per_mat = depth // rows
    full = width // TILE
    widths = [TILE] * full + ([width - full * TILE] if width % TILE else [])
    tiles = len(widths)
    total = chips * tiles

    dp = lax.axis_index("dp")
    z, c = dp // CORES, dp % CORES
    d = 1 - 2 * c
    nxt = lax.rem(z + d + chips, chips) * CORES + c
    prv = lax.rem(z - d + chips, chips) * CORES + c
    par = z * CORES + 1 - c

    def mine(s):
        return lax.rem(z - d * (s + 1) + 2 * chips, chips)

    def theirs(s):
        return lax.rem(z + d * (s + 1) + 2 * chips, chips)

    def columns(j, w):
        return pl.ds(j * TILE if isinstance(j, int) else pl.multiple_of(j * TILE, TILE), w)

    def g_copy(buf, sem, mat, j, w, slot):
        return pltpu.make_async_copy(g_ref.at[0, mat, :, columns(j, w)], buf.at[slot, :, pl.ds(0, w)], sem.at[slot])

    def g_start(buf, sem, chunk, t):
        s, j = t // tiles, t % tiles
        mat = chunk(s) * CORES // per_mat

        @pl.when((t < total) & (j < full))
        def _():
            g_copy(buf, sem, mat, j, TILE, t % 2).start()

        if tiles > full:
            @pl.when((t < total) & (j == full))
            def _():
                g_copy(buf, sem, mat, full, widths[full], t % 2).start()

    some = tokens // STAGES

    def a_copy(mat, k):
        return pltpu.make_async_copy(
            a_ref.at[0, mat, pl.ds(pl.multiple_of(k * some, some), some)], stage.at[k], stage_sem.at[k])

    def transpose(i):
        @pl.loop(0, STAGES)
        def _(k):
            a_copy(order[i], k).wait()
            for b in range(some // KBLOCK):
                span = pl.ds(pl.multiple_of(k * some + b * KBLOCK, KBLOCK), KBLOCK)
                block = stage[k, b * KBLOCK:(b + 1) * KBLOCK, :].T
                for r in range(per_mat):
                    at[order[i] * per_mat + r, :, span] = block[r * rows:(r + 1) * rows]
            if i + 1 < mats:
                a_copy(order[i + 1], k).start()

    spans = [r * rows // LANES * LANES for r in range(per_mat)]
    cover = max(pl.cdiv((r + 1) * rows - spans[r], LANES) * LANES for r in range(per_mat))
    spans = [min(first, depth - cover) for first in spans]

    def early_copy(block, r, n, k):
        return pltpu.make_async_copy(
            a_ref.at[0, block // per_mat, pl.ds(k * some, some), pl.ds(spans[r], cover)],
            stage.at[k, :, pl.ds(n * cover, cover)], early_sem.at[n, k])

    def early_start(block, n):
        for r in range(per_mat):
            @pl.when(block % per_mat == r)
            def _():
                for k in range(STAGES):
                    early_copy(block, r, n, k).start()

    def early_transpose(block, n):
        for r in range(per_mat):
            @pl.when(block % per_mat == r)
            def _():
                for k in range(STAGES):
                    early_copy(block, r, n, k).wait()
                    for b in range(some // KBLOCK):
                        part = stage[k, b * KBLOCK:(b + 1) * KBLOCK, n * cover:(n + 1) * cover].T
                        at[block, :, k * some + b * KBLOCK:k * some + (b + 1) * KBLOCK] = (
                            part[r * rows - spans[r]:(r + 1) * rows - spans[r]])

    def to_partner(t, j, w):
        return pltpu.make_async_remote_copy(
            pbuf.at[j, :, pl.ds(0, w)], pin.at[t % 4, :, pl.ds(0, w)], psend.at[j], precv.at[t % 4],
            device_id={"dp": par}, device_id_type=MESH)

    def place(chunk, core, j, w):
        return x_ref.at[pl.ds(pl.multiple_of((chunk * CORES + core) * rows, rows), rows), columns(j, w)]

    def to_next(s, j, w):
        here = place(mine(s), c, j, w)
        return pltpu.make_async_remote_copy(
            here, here, osend.at[j], rrecv.at[s, j], device_id={"dp": nxt}, device_id_type=MESH)

    def gather(s, j, w):
        here = place(lax.rem(z - d * s + 2 * chips, chips), c, j, w)
        return pltpu.make_async_remote_copy(
            here, here, gsend, grecv.at[s, j], device_id={"dp": nxt}, device_id_type=MESH)

    def share(s, j, w):
        here = place(lax.rem(z - d * s + 2 * chips, chips), c, j, w)
        return pltpu.make_async_remote_copy(
            here, here, dsend, drecv.at[s, j], device_id={"dp": par}, device_id_type=MESH)

    def partner_term(s, j, w):
        t = s * tiles + j
        slot = t % 2
        chunk = theirs(s)
        g_copy(gp, gp_sem, chunk * CORES // per_mat, j, w, slot).wait()

        @pl.when(s > 0)
        def _():
            to_partner(t, j, w).wait_send()

        pbuf[j, :, :w] = jnp.dot(
            at[chunk * CORES + 1 - c], gp[slot, :, :w], preferred_element_type=jnp.float32).astype(jnp.bfloat16)
        to_partner(t, j, w).start()

    def own_term(s, j, w):
        t = s * tiles + j
        slot = t % 2
        chunk = mine(s)
        g_copy(go, go_sem, chunk * CORES // per_mat, j, w, slot).wait()
        acc[:, :w] = jnp.dot(at[chunk * CORES + c], go[slot, :, :w], preferred_element_type=jnp.float32)
        to_partner(t, j, w).wait_recv()

        here = place(chunk, c, j, w)

        @pl.when(s == 0)
        def _():
            here[...] = (acc[:, :w] + pin[t % 4, :, :w].astype(jnp.float32)).astype(jnp.bfloat16)

        @pl.when(s > 0)
        def _():
            to_next(s - 1, j, w).wait()
            here[...] = (
                acc[:, :w] + pin[t % 4, :, :w].astype(jnp.float32) + here[...].astype(jnp.float32)
            ).astype(jnp.bfloat16)

        @pl.when(s < chips - 1)
        def _():
            to_next(s, j, w).start()

        @pl.when(s == chips - 1)
        def _():
            gather(0, j, w).start()
            share(0, j, w).start()

    barrier = pltpu.get_barrier_semaphore()
    for who in (nxt, prv, par):
        pl.semaphore_signal(barrier, inc=1, device_id={"dp": who}, device_id_type=MESH)

    block_p, block_o = theirs(0) * CORES + 1 - c, mine(0) * CORES + c
    early_start(block_p, 0)
    g_start(gp, gp_sem, theirs, 0)
    early_start(block_o, 1)
    g_start(go, go_sem, mine, 0)
    g_start(gp, gp_sem, theirs, 1)
    early_transpose(block_p, 0)
    pl.semaphore_wait(barrier, 3)
    partner_term(0, 0, widths[0])
    early_transpose(block_o, 1)

    base = z * CORES // per_mat
    order = [lax.rem(base + ahead, mats) for ahead in (mats - 1, 1, 2, 0)]
    times = [(0, 1), (0, 4), (1, 1), (2, 1)]
    for k in range(STAGES):
        a_copy(order[0], k).start()

    def step(s, j, w, w_after):
        t = s * tiles + j
        g_start(gp, gp_sem, theirs, t + 2)
        g_start(go, go_sem, mine, t + 1)
        if w_after is None:
            @pl.when(s < chips - 1)
            def _():
                partner_term(s + 1, 0, widths[0])
        else:
            partner_term(s, j + 1, w_after)
        own_term(s, j, w)

    @pl.loop(0, chips)
    def _(s):
        @pl.loop(0, full - 1)
        def _(j):
            step(s, j, TILE, TILE)
            for i, (when_s, when_j) in enumerate(times):
                @pl.when((s == when_s) & (j == when_j))
                def _():
                    transpose(i)

        for j in range(full - 1, tiles):
            step(s, j, widths[j], widths[j + 1] if j + 1 < tiles else None)

    pl.semaphore_signal(clear, inc=1, device_id={"dp": prv}, device_id_type=MESH)
    for j, w in enumerate(widths):
        to_partner((chips - 1) * tiles + j, j, w).wait_send()

    @pl.loop(1, chips)
    def _(s):
        @pl.when(s == chips - 3)
        def _():
            pl.semaphore_wait(clear, 1)

        for j, w in enumerate(widths):
            gather(s - 1, j, w).wait_recv()

            @pl.when(s < chips - 1)
            def _():
                gather(s, j, w).start()

            share(s, j, w).start()
            share(s - 1, j, w).wait_recv()

    for j, w in enumerate(widths):
        share(chips - 1, j, w).wait_recv()

    def all_bytes(chunks, sem):
        part = x_ref.at[pl.ds(0, chunks * rows)]
        pltpu.make_async_copy(part, part, sem).wait()

    all_bytes(chips - 1, gsend)
    all_bytes(chips, dsend)


def writer(x_ref, o_ref, sem):
    part = x_ref.shape[0] // WRITES
    copies = [
        pltpu.make_async_copy(x_ref.at[pl.ds(i * part, part)], o_ref.at[pl.ds(i * part, part)], sem.at[i])
        for i in range(WRITES)
    ]
    for copy in copies:
        copy.start()
    for copy in copies:
        copy.wait()


def solution(mesh):
    members = mesh.shape["dp"]
    chips = members // CORES

    def body(a, g):
        _, mats, tokens, depth = a.shape
        width = g.shape[3]
        rows = mats * depth // members
        tiles = pl.cdiv(width, TILE)
        bf16, f32, dma = jnp.bfloat16, jnp.float32, pltpu.SemaphoreType.DMA
        sums = pl.pallas_call(
            functools.partial(kernel, chips),
            out_shape=pltpu.VMEM((mats * depth, width), bf16),
            in_specs=[pl.BlockSpec(memory_space=pl.ANY)] * 2,
            out_specs=pl.BlockSpec(memory_space=pltpu.VMEM),
            scratch_shapes=[
                pltpu.VMEM((STAGES, tokens // STAGES, depth), bf16),
                pltpu.VMEM((members, rows, tokens), bf16),
                pltpu.VMEM((2, tokens, TILE), bf16),
                pltpu.VMEM((2, tokens, TILE), bf16),
                pltpu.VMEM((rows, TILE), f32),
                pltpu.VMEM((tiles, rows, TILE), bf16),
                pltpu.VMEM((4, rows, TILE), bf16),
                dma((STAGES,)), dma((2, STAGES)), dma((2,)), dma((2,)),
                dma((tiles,)), dma((4,)), dma((tiles,)), dma((chips - 1, tiles)),
                dma, dma,
                dma((chips - 1, tiles)), dma((chips, tiles)),
                pltpu.SemaphoreType.REGULAR,
            ],
            compiler_params=pltpu.CompilerParams(
                collective_id=0, has_side_effects=True, vmem_limit_bytes=30 * 2**20),
        )(a, g)
        out = pl.pallas_call(
            writer,
            out_shape=jax.ShapeDtypeStruct((mats * depth, width), bf16),
            in_specs=[pl.BlockSpec(memory_space=pltpu.VMEM)],
            out_specs=pl.BlockSpec(memory_space=pl.ANY),
            scratch_shapes=[dma((WRITES,))],
            compiler_params=pltpu.CompilerParams(vmem_limit_bytes=2**20),
        )(sums)
        return out.reshape(mats, depth, width)

    part = P(("rep", "dp"))
    return jax.shard_map(body, mesh=mesh, in_specs=(part, part), out_specs=P("rep"), check_vma=False)
```

```python
import functools

import jax
import jax.numpy as jnp
from jax import lax
from jax.experimental import pallas as pl
from jax.experimental.pallas import tpu as pltpu
from jax.sharding import PartitionSpec as P

MESH = pl.DeviceIdType.MESH
CORES = 2
TILE = 512
KBLOCK = 256
STAGES = 4
LANES = 128
WRITES = 16


def kernel(chips, a_ref, g_ref, x_ref, stage, at, gp, go, acc, pbuf, pin,
           stage_sem, early_sem, gp_sem, go_sem, psend, precv, osend, rrecv, gsend, dsend, grecv, drecv, clear):
    _, mats, tokens, depth = a_ref.shape
    width = g_ref.shape[3]
    rows = at.shape[1]
    per_mat = depth // rows
    full = width // TILE
    widths = [TILE] * full + ([width - full * TILE] if width % TILE else [])
    tiles = len(widths)
    total = chips * tiles

    dp = lax.axis_index("dp")
    z, c = dp // CORES, dp % CORES
    d = 1 - 2 * c
    nxt = lax.rem(z + d + chips, chips) * CORES + c
    prv = lax.rem(z - d + chips, chips) * CORES + c
    par = z * CORES + 1 - c
    beyond = lax.rem(z + d + chips, chips) * CORES + 1 - c

    def mine(s):
        return lax.rem(z - d * (s + 1) + 2 * chips, chips)

    def theirs(s):
        return lax.rem(z + d * (s + 1) + 2 * chips, chips)

    def columns(j, w):
        return pl.ds(j * TILE if isinstance(j, int) else pl.multiple_of(j * TILE, TILE), w)

    def g_copy(buf, sem, mat, j, w, slot):
        return pltpu.make_async_copy(g_ref.at[0, mat, :, columns(j, w)], buf.at[slot, :, pl.ds(0, w)], sem.at[slot])

    def g_start(buf, sem, chunk, t):
        s, j = t // tiles, t % tiles
        mat = chunk(s) * CORES // per_mat

        @pl.when((t < total) & (j < full))
        def _():
            g_copy(buf, sem, mat, j, TILE, t % 2).start()

        if tiles > full:
            @pl.when((t < total) & (j == full))
            def _():
                g_copy(buf, sem, mat, full, widths[full], t % 2).start()

    some = tokens // STAGES

    def a_copy(mat, k):
        return pltpu.make_async_copy(
            a_ref.at[0, mat, pl.ds(pl.multiple_of(k * some, some), some)], stage.at[k], stage_sem.at[k])

    def transpose(i):
        @pl.loop(0, STAGES)
        def _(k):
            a_copy(order[i], k).wait()
            for b in range(some // KBLOCK):
                span = pl.ds(pl.multiple_of(k * some + b * KBLOCK, KBLOCK), KBLOCK)
                block = stage[k, b * KBLOCK:(b + 1) * KBLOCK, :].T
                for r in range(per_mat):
                    at[order[i] * per_mat + r, :, span] = block[r * rows:(r + 1) * rows]
            if i + 1 < mats:
                a_copy(order[i + 1], k).start()

    spans = [r * rows // LANES * LANES for r in range(per_mat)]
    cover = max(pl.cdiv((r + 1) * rows - spans[r], LANES) * LANES for r in range(per_mat))
    spans = [min(first, depth - cover) for first in spans]

    def early_copy(block, r, n, k):
        return pltpu.make_async_copy(
            a_ref.at[0, block // per_mat, pl.ds(k * some, some), pl.ds(spans[r], cover)],
            stage.at[k, :, pl.ds(n * cover, cover)], early_sem.at[n, k])

    def early_start(block, n):
        for r in range(per_mat):
            @pl.when(block % per_mat == r)
            def _():
                for k in range(STAGES):
                    early_copy(block, r, n, k).start()

    def early_transpose(block, n, meanwhile=lambda: None):
        for r in range(per_mat):
            @pl.when(block % per_mat == r)
            def _():
                for k in range(STAGES):
                    early_copy(block, r, n, k).wait()
                    if k == 0:
                        meanwhile()
                    for b in range(some // KBLOCK):
                        part = stage[k, b * KBLOCK:(b + 1) * KBLOCK, n * cover:(n + 1) * cover].T
                        at[block, :, k * some + b * KBLOCK:k * some + (b + 1) * KBLOCK] = (
                            part[r * rows - spans[r]:(r + 1) * rows - spans[r]])

    def to_partner(t, j, w):
        return pltpu.make_async_remote_copy(
            pbuf.at[j, :, pl.ds(0, w)], pin.at[t % 4, :, pl.ds(0, w)], psend.at[j], precv.at[t % 4],
            device_id={"dp": par}, device_id_type=MESH)

    def place(chunk, core, j, w):
        return x_ref.at[pl.ds(pl.multiple_of((chunk * CORES + core) * rows, rows), rows), columns(j, w)]

    def to_next(s, j, w):
        here = place(mine(s), c, j, w)
        return pltpu.make_async_remote_copy(
            here, here, osend.at[j], rrecv.at[s, j], device_id={"dp": nxt}, device_id_type=MESH)

    def gather(s, j, w):
        here = place(lax.rem(z - d * s + 2 * chips, chips), c, j, w)
        return pltpu.make_async_remote_copy(
            here, here, gsend, grecv.at[s, j], device_id={"dp": nxt}, device_id_type=MESH)

    def share(s, j, w):
        here = place(lax.rem(z - d * s + 2 * chips, chips), c, j, w)
        return pltpu.make_async_remote_copy(
            here, here, dsend, drecv.at[s, j], device_id={"dp": par}, device_id_type=MESH)

    def last_share(w):
        here = place(lax.rem(z - d * (chips - 2) + 2 * chips, chips), c, tiles - 1, w)
        return pltpu.make_async_remote_copy(
            here, here, dsend, drecv.at[chips - 1, tiles - 1], device_id={"dp": beyond}, device_id_type=MESH)

    def partner_term(s, j, w):
        t = s * tiles + j
        slot = t % 2
        chunk = theirs(s)
        g_copy(gp, gp_sem, chunk * CORES // per_mat, j, w, slot).wait()

        @pl.when(s > 0)
        def _():
            to_partner(t, j, w).wait_send()

        pbuf[j, :, :w] = jnp.dot(
            at[chunk * CORES + 1 - c], gp[slot, :, :w], preferred_element_type=jnp.float32).astype(jnp.bfloat16)
        to_partner(t, j, w).start()

    def own_term(s, j, w):
        t = s * tiles + j
        slot = t % 2
        chunk = mine(s)
        g_copy(go, go_sem, chunk * CORES // per_mat, j, w, slot).wait()
        acc[:, :w] = jnp.dot(at[chunk * CORES + c], go[slot, :, :w], preferred_element_type=jnp.float32)
        to_partner(t, j, w).wait_recv()

        here = place(chunk, c, j, w)

        @pl.when(s == 0)
        def _():
            here[...] = (acc[:, :w] + pin[t % 4, :, :w].astype(jnp.float32)).astype(jnp.bfloat16)

        @pl.when(s > 0)
        def _():
            to_next(s - 1, j, w).wait()
            here[...] = (
                acc[:, :w] + pin[t % 4, :, :w].astype(jnp.float32) + here[...].astype(jnp.float32)
            ).astype(jnp.bfloat16)

        @pl.when(s < chips - 1)
        def _():
            to_next(s, j, w).start()

        @pl.when(s == chips - 1)
        def _():
            gather(0, j, w).start()
            share(0, j, w).start()

    barrier = pltpu.get_barrier_semaphore()
    for who in (nxt, prv, par, beyond):
        pl.semaphore_signal(barrier, inc=1, device_id={"dp": who}, device_id_type=MESH)

    block_p, block_o = theirs(0) * CORES + 1 - c, mine(0) * CORES + c
    early_start(block_p, 0)
    g_start(gp, gp_sem, theirs, 0)
    early_start(block_o, 1)
    early_transpose(block_p, 0, lambda: g_start(go, go_sem, mine, 0))
    g_start(gp, gp_sem, theirs, 1)
    pl.semaphore_wait(barrier, 4)
    partner_term(0, 0, widths[0])
    early_transpose(block_o, 1)

    base = z * CORES // per_mat
    order = [lax.rem(base + ahead, mats) for ahead in (mats - 1, 1, 2, 0)]
    times = [(0, 1), (0, 4), (1, 1), (2, 1)]
    for k in range(STAGES):
        a_copy(order[0], k).start()

    g_start(gp, gp_sem, theirs, 2)
    g_start(go, go_sem, mine, 1)
    own_term(0, 0, widths[0])
    partner_term(0, 1, widths[1])

    def step(s, j, w, w_after):
        t = s * tiles + j
        g_start(gp, gp_sem, theirs, t + 2)
        g_start(go, go_sem, mine, t + 1)
        if w_after is None:
            @pl.when(s < chips - 1)
            def _():
                partner_term(s + 1, 0, widths[0])
        else:
            partner_term(s, j + 1, w_after)
        own_term(s, j, w)

    @pl.loop(0, chips)
    def _(s):
        @pl.loop(0, full - 1)
        def _(j):
            @pl.when(s + j > 0)
            def _():
                step(s, j, TILE, TILE)

            for i, (when_s, when_j) in enumerate(times):
                @pl.when((s == when_s) & (j == when_j))
                def _():
                    transpose(i)

        for j in range(full - 1, tiles):
            step(s, j, widths[j], widths[j + 1] if j + 1 < tiles else None)

    pl.semaphore_signal(clear, inc=1, device_id={"dp": prv}, device_id_type=MESH)
    for j, w in enumerate(widths):
        to_partner((chips - 1) * tiles + j, j, w).wait_send()

    @pl.loop(1, chips)
    def _(s):
        @pl.when(s == chips - 3)
        def _():
            pl.semaphore_wait(clear, 1)

        for j, w in enumerate(widths):
            gather(s - 1, j, w).wait_recv()

            @pl.when(s < chips - 1)
            def _():
                gather(s, j, w).start()

            if j == tiles - 1:
                @pl.when(s == chips - 2)
                def _():
                    last_share(w).start()

                @pl.when(s < chips - 1)
                def _():
                    share(s, j, w).start()
            else:
                share(s, j, w).start()
            share(s - 1, j, w).wait_recv()

    for j, w in enumerate(widths):
        share(chips - 1, j, w).wait_recv()

    def all_bytes(chunks, sem):
        part = x_ref.at[pl.ds(0, chunks * rows)]
        pltpu.make_async_copy(part, part, sem).wait()

    all_bytes(chips - 1, gsend)
    all_bytes(chips, dsend)


def writer(x_ref, o_ref, sem):
    part = x_ref.shape[0] // WRITES
    copies = [
        pltpu.make_async_copy(x_ref.at[pl.ds(i * part, part)], o_ref.at[pl.ds(i * part, part)], sem.at[i])
        for i in range(WRITES)
    ]
    for copy in copies:
        copy.start()
    for copy in copies:
        copy.wait()


def solution(mesh):
    members = mesh.shape["dp"]
    chips = members // CORES

    def body(a, g):
        _, mats, tokens, depth = a.shape
        width = g.shape[3]
        rows = mats * depth // members
        tiles = pl.cdiv(width, TILE)
        bf16, f32, dma = jnp.bfloat16, jnp.float32, pltpu.SemaphoreType.DMA
        sums = pl.pallas_call(
            functools.partial(kernel, chips),
            out_shape=pltpu.VMEM((mats * depth, width), bf16),
            in_specs=[pl.BlockSpec(memory_space=pl.ANY)] * 2,
            out_specs=pl.BlockSpec(memory_space=pltpu.VMEM),
            scratch_shapes=[
                pltpu.VMEM((STAGES, tokens // STAGES, depth), bf16),
                pltpu.VMEM((members, rows, tokens), bf16),
                pltpu.VMEM((2, tokens, TILE), bf16),
                pltpu.VMEM((2, tokens, TILE), bf16),
                pltpu.VMEM((rows, TILE), f32),
                pltpu.VMEM((tiles, rows, TILE), bf16),
                pltpu.VMEM((4, rows, TILE), bf16),
                dma((STAGES,)), dma((2, STAGES)), dma((2,)), dma((2,)),
                dma((tiles,)), dma((4,)), dma((tiles,)), dma((chips - 1, tiles)),
                dma, dma,
                dma((chips - 1, tiles)), dma((chips, tiles)),
                pltpu.SemaphoreType.REGULAR,
            ],
            compiler_params=pltpu.CompilerParams(
                collective_id=0, has_side_effects=True, vmem_limit_bytes=30 * 2**20),
        )(a, g)
        out = pl.pallas_call(
            writer,
            out_shape=jax.ShapeDtypeStruct((mats * depth, width), bf16),
            in_specs=[pl.BlockSpec(memory_space=pltpu.VMEM)],
            out_specs=pl.BlockSpec(memory_space=pl.ANY),
            scratch_shapes=[dma((WRITES,))],
            compiler_params=pltpu.CompilerParams(vmem_limit_bytes=2**20),
        )(sums)
        return out.reshape(mats, depth, width)

    part = P(("rep", "dp"))
    return jax.shard_map(body, mesh=mesh, in_specs=(part, part), out_specs=P("rep"), check_vma=False)
```

```python
import functools

import jax
import jax.numpy as jnp
from jax import lax
from jax.experimental import pallas as pl
from jax.experimental.pallas import tpu as pltpu
from jax.sharding import PartitionSpec as P

MESH = pl.DeviceIdType.MESH
CORES = 2
TILE = 512
KBLOCK = 256
STAGES = 4
LANES = 128
WRITES = 16


def kernel(chips, a_ref, g_ref, x_ref, stage, at, gp, go, acc, pbuf, pin,
           stage_sem, early_sem, gp_sem, go_sem, psend, precv, osend, rrecv, gsend, dsend, grecv, drecv, clear):
    _, mats, tokens, depth = a_ref.shape
    width = g_ref.shape[3]
    rows = at.shape[1]
    per_mat = depth // rows
    full = width // TILE
    widths = [TILE] * full + ([width - full * TILE] if width % TILE else [])
    tiles = len(widths)
    total = chips * tiles

    dp = lax.axis_index("dp")
    z, c = dp // CORES, dp % CORES
    d = 1 - 2 * c
    nxt = lax.rem(z + d + chips, chips) * CORES + c
    prv = lax.rem(z - d + chips, chips) * CORES + c
    par = z * CORES + 1 - c
    beyond = lax.rem(z + d + chips, chips) * CORES + 1 - c

    def mine(s):
        return lax.rem(z - d * (s + 1) + 2 * chips, chips)

    def theirs(s):
        return lax.rem(z + d * (s + 1) + 2 * chips, chips)

    def columns(j, w):
        return pl.ds(j * TILE if isinstance(j, int) else pl.multiple_of(j * TILE, TILE), w)

    def g_copy(buf, sem, mat, j, w, slot):
        return pltpu.make_async_copy(g_ref.at[0, mat, :, columns(j, w)], buf.at[slot, :, pl.ds(0, w)], sem.at[slot])

    def g_start(buf, sem, chunk, t):
        s, j = t // tiles, t % tiles
        mat = chunk(s) * CORES // per_mat

        @pl.when((t < total) & (j < full))
        def _():
            g_copy(buf, sem, mat, j, TILE, t % 2).start()

        if tiles > full:
            @pl.when((t < total) & (j == full))
            def _():
                g_copy(buf, sem, mat, full, widths[full], t % 2).start()

    some = tokens // STAGES

    def a_copy(mat, k):
        return pltpu.make_async_copy(
            a_ref.at[0, mat, pl.ds(pl.multiple_of(k * some, some), some)], stage.at[k], stage_sem.at[k])

    def transpose(i):
        @pl.loop(0, STAGES)
        def _(k):
            a_copy(order[i], k).wait()
            for b in range(some // KBLOCK):
                span = pl.ds(pl.multiple_of(k * some + b * KBLOCK, KBLOCK), KBLOCK)
                block = stage[k, b * KBLOCK:(b + 1) * KBLOCK, :].T
                for r in range(per_mat):
                    at[order[i] * per_mat + r, :, span] = block[r * rows:(r + 1) * rows]
            if i + 1 < mats:
                a_copy(order[i + 1], k).start()

    spans = [r * rows // LANES * LANES for r in range(per_mat)]
    cover = max(pl.cdiv((r + 1) * rows - spans[r], LANES) * LANES for r in range(per_mat))
    spans = [min(first, depth - cover) for first in spans]

    def early_copy(block, r, n, k):
        return pltpu.make_async_copy(
            a_ref.at[0, block // per_mat, pl.ds(k * some, some), pl.ds(spans[r], cover)],
            stage.at[k, :, pl.ds(n * cover, cover)], early_sem.at[n, k])

    def early_start(block, n):
        for r in range(per_mat):
            @pl.when(block % per_mat == r)
            def _():
                for k in range(STAGES):
                    early_copy(block, r, n, k).start()

    def early_transpose(block, n, meanwhile=lambda: None):
        for r in range(per_mat):
            @pl.when(block % per_mat == r)
            def _():
                for k in range(STAGES):
                    early_copy(block, r, n, k).wait()
                    if k == 0:
                        meanwhile()
                    for b in range(some // KBLOCK):
                        part = stage[k, b * KBLOCK:(b + 1) * KBLOCK, n * cover:(n + 1) * cover].T
                        at[block, :, k * some + b * KBLOCK:k * some + (b + 1) * KBLOCK] = (
                            part[r * rows - spans[r]:(r + 1) * rows - spans[r]])

    def to_partner(t, j, w):
        return pltpu.make_async_remote_copy(
            pbuf.at[j, :, pl.ds(0, w)], pin.at[t % 4, :, pl.ds(0, w)], psend.at[j], precv.at[t % 4],
            device_id={"dp": par}, device_id_type=MESH)

    def place(chunk, core, j, w):
        return x_ref.at[pl.ds(pl.multiple_of((chunk * CORES + core) * rows, rows), rows), columns(j, w)]

    def to_next(s, j, w):
        here = place(mine(s), c, j, w)
        return pltpu.make_async_remote_copy(
            here, here, osend.at[j], rrecv.at[s, j], device_id={"dp": nxt}, device_id_type=MESH)

    def gather(s, j, w):
        here = place(lax.rem(z - d * s + 2 * chips, chips), c, j, w)
        return pltpu.make_async_remote_copy(
            here, here, gsend, grecv.at[s, j], device_id={"dp": nxt}, device_id_type=MESH)

    def share(s, j, w):
        here = place(lax.rem(z - d * s + 2 * chips, chips), c, j, w)
        return pltpu.make_async_remote_copy(
            here, here, dsend, drecv.at[s, j], device_id={"dp": par}, device_id_type=MESH)

    def last_share(w):
        here = place(lax.rem(z - d * (chips - 2) + 2 * chips, chips), c, tiles - 1, w)
        return pltpu.make_async_remote_copy(
            here, here, dsend, drecv.at[chips - 1, tiles - 1], device_id={"dp": beyond}, device_id_type=MESH)

    def partner_term(s, j, w):
        t = s * tiles + j
        slot = t % 2
        chunk = theirs(s)
        g_copy(gp, gp_sem, chunk * CORES // per_mat, j, w, slot).wait()

        @pl.when(s > 0)
        def _():
            to_partner(t, j, w).wait_send()

        pbuf[j, :, :w] = jnp.dot(
            at[chunk * CORES + 1 - c], gp[slot, :, :w], preferred_element_type=jnp.float32).astype(jnp.bfloat16)
        to_partner(t, j, w).start()

    def own_term(s, j, w):
        t = s * tiles + j
        slot = t % 2
        chunk = mine(s)
        g_copy(go, go_sem, chunk * CORES // per_mat, j, w, slot).wait()
        acc[:, :w] = jnp.dot(at[chunk * CORES + c], go[slot, :, :w], preferred_element_type=jnp.float32)
        to_partner(t, j, w).wait_recv()

        here = place(chunk, c, j, w)

        @pl.when(s == 0)
        def _():
            here[...] = (acc[:, :w] + pin[t % 4, :, :w].astype(jnp.float32)).astype(jnp.bfloat16)

        @pl.when(s > 0)
        def _():
            to_next(s - 1, j, w).wait()
            here[...] = (
                acc[:, :w] + pin[t % 4, :, :w].astype(jnp.float32) + here[...].astype(jnp.float32)
            ).astype(jnp.bfloat16)

        @pl.when(s < chips - 1)
        def _():
            to_next(s, j, w).start()

        @pl.when(s == chips - 1)
        def _():
            gather(0, j, w).start()
            share(0, j, w).start()

    barrier = pltpu.get_barrier_semaphore()
    for who in (nxt, prv, par, beyond):
        pl.semaphore_signal(barrier, inc=1, device_id={"dp": who}, device_id_type=MESH)

    block_p, block_o = theirs(0) * CORES + 1 - c, mine(0) * CORES + c
    early_start(block_p, 0)
    g_start(gp, gp_sem, theirs, 0)
    early_start(block_o, 1)
    early_transpose(block_p, 0, lambda: g_start(go, go_sem, mine, 0))
    g_start(gp, gp_sem, theirs, 1)
    pl.semaphore_wait(barrier, 4)
    partner_term(0, 0, widths[0])
    early_transpose(block_o, 1)

    base = z * CORES // per_mat
    order = [lax.rem(base + ahead, mats) for ahead in (mats - 1, 1, 2, 0)]
    times = [(0, 5), (0, 7), (1, 5), (2, 5)]

    g_start(gp, gp_sem, theirs, 2)
    g_start(go, go_sem, mine, 1)
    own_term(0, 0, widths[0])
    partner_term(0, 1, widths[1])

    def step(s, j, w, w_after):
        t = s * tiles + j
        g_start(gp, gp_sem, theirs, t + 2)
        g_start(go, go_sem, mine, t + 1)
        if w_after is None:
            @pl.when(s < chips - 1)
            def _():
                partner_term(s + 1, 0, widths[0])
        else:
            partner_term(s, j + 1, w_after)
        own_term(s, j, w)

    @pl.loop(0, chips)
    def _(s):
        @pl.loop(0, full - 1)
        def _(j):
            @pl.when(s + j > 0)
            def _():
                step(s, j, TILE, TILE)

            @pl.when((s == 0) & (j == times[0][1] - 2))
            def _():
                for k in range(STAGES):
                    a_copy(order[0], k).start()

            for i, (when_s, when_j) in enumerate(times):
                @pl.when((s == when_s) & (j == when_j))
                def _():
                    transpose(i)

        for j in range(full - 1, tiles):
            step(s, j, widths[j], widths[j + 1] if j + 1 < tiles else None)

    pl.semaphore_signal(clear, inc=1, device_id={"dp": prv}, device_id_type=MESH)
    for j, w in enumerate(widths):
        to_partner((chips - 1) * tiles + j, j, w).wait_send()

    @pl.loop(1, chips)
    def _(s):
        @pl.when(s == chips - 3)
        def _():
            pl.semaphore_wait(clear, 1)

        for j, w in enumerate(widths):
            gather(s - 1, j, w).wait_recv()

            @pl.when(s < chips - 1)
            def _():
                gather(s, j, w).start()

            if j == tiles - 1:
                @pl.when(s == chips - 2)
                def _():
                    last_share(w).start()

                @pl.when(s < chips - 1)
                def _():
                    share(s, j, w).start()
            else:
                share(s, j, w).start()
            share(s - 1, j, w).wait_recv()

    for j, w in enumerate(widths):
        share(chips - 1, j, w).wait_recv()

    def all_bytes(chunks, sem):
        part = x_ref.at[pl.ds(0, chunks * rows)]
        pltpu.make_async_copy(part, part, sem).wait()

    all_bytes(chips - 1, gsend)
    all_bytes(chips, dsend)


def writer(x_ref, o_ref, sem):
    part = x_ref.shape[0] // WRITES
    copies = [
        pltpu.make_async_copy(x_ref.at[pl.ds(i * part, part)], o_ref.at[pl.ds(i * part, part)], sem.at[i])
        for i in range(WRITES)
    ]
    for copy in copies:
        copy.start()
    for copy in copies:
        copy.wait()


def solution(mesh):
    members = mesh.shape["dp"]
    chips = members // CORES

    def body(a, g):
        _, mats, tokens, depth = a.shape
        width = g.shape[3]
        rows = mats * depth // members
        tiles = pl.cdiv(width, TILE)
        bf16, f32, dma = jnp.bfloat16, jnp.float32, pltpu.SemaphoreType.DMA
        sums = pl.pallas_call(
            functools.partial(kernel, chips),
            out_shape=pltpu.VMEM((mats * depth, width), bf16),
            in_specs=[pl.BlockSpec(memory_space=pl.ANY)] * 2,
            out_specs=pl.BlockSpec(memory_space=pltpu.VMEM),
            scratch_shapes=[
                pltpu.VMEM((STAGES, tokens // STAGES, depth), bf16),
                pltpu.VMEM((members, rows, tokens), bf16),
                pltpu.VMEM((2, tokens, TILE), bf16),
                pltpu.VMEM((2, tokens, TILE), bf16),
                pltpu.VMEM((rows, TILE), f32),
                pltpu.VMEM((tiles, rows, TILE), bf16),
                pltpu.VMEM((4, rows, TILE), bf16),
                dma((STAGES,)), dma((2, STAGES)), dma((2,)), dma((2,)),
                dma((tiles,)), dma((4,)), dma((tiles,)), dma((chips - 1, tiles)),
                dma, dma,
                dma((chips - 1, tiles)), dma((chips, tiles)),
                pltpu.SemaphoreType.REGULAR,
            ],
            compiler_params=pltpu.CompilerParams(
                collective_id=0, has_side_effects=True, vmem_limit_bytes=30 * 2**20),
        )(a, g)
        out = pl.pallas_call(
            writer,
            out_shape=jax.ShapeDtypeStruct((mats * depth, width), bf16),
            in_specs=[pl.BlockSpec(memory_space=pltpu.VMEM)],
            out_specs=pl.BlockSpec(memory_space=pl.ANY),
            scratch_shapes=[dma((WRITES,))],
            compiler_params=pltpu.CompilerParams(vmem_limit_bytes=2**20),
        )(sums)
        return out.reshape(mats, depth, width)

    part = P(("rep", "dp"))
    return jax.shard_map(body, mesh=mesh, in_specs=(part, part), out_specs=P("rep"), check_vma=False)
```
